32 devices in a mesh: dp: 8 (over z, core), mp: 4 (over y, x).
Axes of the slice: x: 2, y: 2, z: 4, core: 2. Of those that a mesh axis runs over, the one named last changes fastest.
Arguments:
- patches: bfloat16 [256, 256, 1280], P(('dp', 'mp')), may hold values from -6 to 6
- position: bfloat16 [256, 1280], replicated, may hold values from -3 to 3
- keep: int32 [256, 64], P(('dp', 'mp')), may hold values from 0 to 255, as said below
- counts: int32 [256], replicated, may hold values from 1 to 64, as said below
- offsets: int32 [256], replicated, may hold values from 0 to 10239, as said below
- ln_gain: float32 [1, 2, 1280], replicated, may hold values from 0.25 to 1.75
- ln_bias: float32 [1, 2, 1280], replicated, may hold values from -2 to 2
- w_qkv: bfloat16 [1, 3, 1280, 1280], P(None, None, 'dp', 'mp')
- b_qkv: float32 [1, 3, 1280], P(None, None, 'mp'), may hold values from -3 to 3
- w_o: bfloat16 [1, 1280, 1280], P(None, 'mp', 'dp'), may hold values from -0.15625 to 0.15625
- b_o: float32 [1, 1280], replicated, may hold values from -1.5 to 1.5
- w_up: bfloat16 [1, 1280, 5120], P(None, 'dp', 'mp'), may hold values from -0.15625 to 0.15625
- b_up: float32 [1, 5120], P(None, 'mp'), may hold values from -3 to 3
- w_down: bfloat16 [1, 5120, 1280], P(None, 'mp', 'dp'), may hold values from -0.078125 to 0.078125
- b_down: float32 [1, 1280], replicated, may hold values from -1.5 to 1.5
Outputs:
- encoded: bfloat16 [10240, 1280], P(('dp', 'mp'))
The draws below stay inside these ranges and needn't reach their ends.
Inputs may be any that keep to these rules, and one draw needn't show every extreme that they name: `keep`: the first counts[i] entries of row i are distinct and name image i's visible patches; later entries are unused. `counts`: some image has exactly 64 visible patches. Image i, held by dp index s = i // 32, occupies packed rows offsets[i] to offsets[i] + counts[i] - 1, all inside the aligned block of 160 rows numbered d * 8 + s for some shard d; no two images share a row.
All inputs are finite; a program needn't handle non-finite values.
Results may differ from the reference program's by a relative error of at most 0.015.
Values may be sent and summed in bfloat16 or wider, within the bound.
A program may use at most 64 MiB of HBM per device.

```python
import math
import jax
import jax.numpy as jnp
from jax import lax

D = 1280
HEADS = 16
HEAD = 80
FF = 5120
PATCHES = 256
KEEP_MAX = 64
LAYERS = 1
IMG_DEV = 32
IMAGES = 256
SLOT = 160
PACK_DEV = 1280
PACKED = 10240
N_MP = 4


def packing_plan(key):
    shard_total = IMAGES // IMG_DEV
    key_order, key_raw, key_cap, key_force = jax.random.split(jax.random.fold_in(key, 71), 4)
    order = jax.vmap(lambda subkey: jax.random.permutation(subkey, IMG_DEV))(jax.random.split(key_order, shard_total)).astype(jnp.int32)
    destination = order % shard_total
    rank_in = order // shard_total
    lowest = max(1, KEEP_MAX // 8)
    ceiling = jax.random.randint(key_cap, (shard_total, 1), lowest, KEEP_MAX + 1)
    raw_count = jnp.minimum(jax.random.randint(key_raw, (shard_total, IMG_DEV), lowest, KEEP_MAX + 1), ceiling)
    mates = destination[:, :, None] == destination[:, None, :]
    mate_total = jnp.sum(jnp.where(mates, raw_count[:, None, :], 0), axis=-1)
    mate_number = jnp.sum(mates.astype(jnp.int32), axis=-1)
    room = SLOT - mate_number
    scaled = 1 + (raw_count - 1) * room // jnp.maximum(mate_total - mate_number, room)
    forced_source = jax.random.randint(key_force, (), 0, shard_total)
    source_ids = jnp.arange(shard_total, dtype=jnp.int32)[:, None]
    in_source = source_ids == forced_source
    chosen = in_source & (order == 0)
    partner = in_source & (destination == 0)
    counts_grid = jnp.where(chosen, KEEP_MAX, jnp.where(partner, 1, scaled))
    earlier = mates & (rank_in[:, None, :] < rank_in[:, :, None])
    before = jnp.sum(jnp.where(earlier, counts_grid[:, None, :], 0), axis=-1)
    offsets_grid = destination * PACK_DEV + source_ids * SLOT + before
    return (counts_grid.reshape(IMAGES).astype(jnp.int32), offsets_grid.reshape(IMAGES).astype(jnp.int32))


def draw_counts(key, part):
    return packing_plan(key)[0]


def draw_offsets(key, part):
    return packing_plan(key)[1]


def draw_keep(key, part):
    subkeys = jax.random.split(jax.random.fold_in(key, 13), IMAGES)
    return jax.vmap(lambda subkey: jax.random.permutation(subkey, PATCHES)[:KEEP_MAX])(subkeys).astype(jnp.int32)


def draw_w_qkv(key, part):
    key_base = jax.random.fold_in(jax.random.fold_in(key, 29), 0)
    matrices = jax.random.normal(key_base, (LAYERS, 3, D, D), jnp.float32) / math.sqrt(D)
    return matrices.astype(jnp.bfloat16)


def levels(rng, extent, cuts, low, largest):
    level, own = 1.0, jax.random.fold_in(rng, 6)
    for dim, blocks in cuts:
        steps = jnp.exp(jax.random.uniform(jax.random.fold_in(own, dim), (blocks,), jnp.float32, low / len(cuts), largest / len(cuts)))
        level = level * jnp.repeat(steps, extent[dim] // blocks).reshape([-1 if axis == dim else 1 for axis in range(len(extent))])
    return level


def bell_draw(rng, extent, deviation, limit, cuts=(), kind=jnp.bfloat16):
    result = jax.random.normal(rng, extent, jnp.float32) * deviation
    if len(cuts) > 0:
        result = levels(rng, extent, cuts, -0.22, 0.18) * result
    return jnp.clip(result, min=-limit, max=limit).astype(kind)


def setup_inputs(seed: int = 0) -> dict:
    keys = jax.random.split(jax.random.key(seed), 16)
    return {
        "patches": bell_draw(keys[0], (IMAGES, PATCHES, D), 1.0, 6.0, ((0, 32),)),
        "position": bell_draw(keys[1], (PATCHES, D), 0.5, 3.0),
        "keep": draw_keep(jax.random.fold_in(keys[15], 71), 0),
        "counts": draw_counts(jax.random.fold_in(keys[15], 71), 0),
        "offsets": draw_offsets(jax.random.fold_in(keys[15], 71), 0),
        "ln_gain": jnp.clip(1.0 + 0.15 * jax.random.normal(keys[5], (LAYERS, 2, D), jnp.float32), 0.25, 1.75),
        "ln_bias": bell_draw(keys[6], (LAYERS, 2, D), 0.3, 2.0, (), jnp.float32),
        "w_qkv": draw_w_qkv(jax.random.fold_in(keys[15], 71), 0),
        "b_qkv": bell_draw(keys[8], (LAYERS, 3, D), 0.5, 3.0, ((2, 4),), jnp.float32),
        "w_o": bell_draw(keys[9], (LAYERS, D, D), D ** -0.5, 0.15625, ((1, 4), (2, 8))),
        "b_o": bell_draw(keys[10], (LAYERS, D), 0.2, 1.5, (), jnp.float32),
        "w_up": bell_draw(keys[11], (LAYERS, D, FF), D ** -0.5, 0.15625, ((1, 8), (2, 4))),
        "b_up": bell_draw(keys[12], (LAYERS, FF), 0.5, 3.0, ((1, 4),), jnp.float32),
        "w_down": bell_draw(keys[13], (LAYERS, FF, D), FF ** -0.5, 0.078125, ((1, 4), (2, 8))),
        "b_down": bell_draw(keys[14], (LAYERS, D), 0.2, 1.5, (), jnp.float32),
    }


def layer_norm(values, gain_row, shift_row):
    row_mean = lax.optimization_barrier(jnp.mean(values, axis=-1, keepdims=True))
    centred = values - row_mean
    spread = lax.optimization_barrier(jnp.mean(centred * centred, axis=-1, keepdims=True))
    return (centred * lax.rsqrt(spread + 1e-06) * gain_row + shift_row).astype(jnp.bfloat16)

def split_sum(left, weight, groups):
    group_width = left.shape[1] // groups
    running = jnp.zeros((left.shape[0], weight.shape[1]), jnp.float32)
    for group_index in range(groups):
        partial_value = jnp.dot(left[:, group_index * group_width:(group_index + 1) * group_width], weight[group_index * group_width:(group_index + 1) * group_width], preferred_element_type=jnp.float32)
        rounded = lax.optimization_barrier(partial_value.astype(jnp.bfloat16))
        running = running + rounded.astype(jnp.float32)
    return running

def shard_attention(pieces):
    queries, key_rows, value_rows, labels_shard = pieces
    scores = jnp.einsum('qhe,khe->hqk', queries.astype(jnp.float32), key_rows.astype(jnp.float32)) * (1.0 / math.sqrt(HEAD))
    matches = labels_shard[:, None] == labels_shard[None, :]
    scores = jnp.where(matches[None], scores, -jnp.inf)
    row_max = lax.optimization_barrier(jnp.max(scores, axis=-1, keepdims=True))
    weights = jnp.exp(scores - row_max)
    probabilities = (weights / lax.optimization_barrier(jnp.sum(weights, axis=-1, keepdims=True))).astype(jnp.bfloat16)
    attended = jnp.einsum('hqk,khe->qhe', probabilities.astype(jnp.float32), value_rows.astype(jnp.float32))
    return attended.astype(jnp.bfloat16)

def reference(patches, position, keep, counts, offsets, ln_gain, ln_bias, w_qkv, b_qkv, w_o, b_o, w_up, b_up, w_down, b_down):
    picked = jnp.take_along_axis(patches, keep[:, :, None], axis=1)
    placed = jnp.take(position, keep, axis=0)
    tokens = (picked.astype(jnp.float32) + placed.astype(jnp.float32)).astype(jnp.bfloat16)
    positions_in = jnp.arange(KEEP_MAX, dtype=jnp.int32)
    is_live = positions_in[None, :] < counts[:, None]
    target = jnp.where(is_live, offsets[:, None] + positions_in[None, :], PACKED).reshape(-1)
    stream = jnp.zeros((PACKED, D), jnp.bfloat16).at[target].set(tokens.reshape(-1, D), mode='drop')
    packed_rows = jnp.arange(PACKED, dtype=jnp.int32)
    image_ids = jnp.arange(counts.shape[0], dtype=jnp.int32)
    inside = (packed_rows[:, None] >= offsets[None, :]) & (packed_rows[:, None] < (offsets + counts)[None, :])
    labels = lax.optimization_barrier(jnp.max(jnp.where(inside, image_ids[None, :] + 1, 0), axis=1)) - 1
    shard_total = PACKED // PACK_DEV
    for layer_index in range(LAYERS):
        normed = layer_norm(stream.astype(jnp.float32), ln_gain[layer_index, 0], ln_bias[layer_index, 0])
        projected = (jnp.einsum('rd,tdc->trc', normed.astype(jnp.float32), w_qkv[layer_index].astype(jnp.float32)) + b_qkv[layer_index][:, None, :]).astype(jnp.bfloat16)
        shaped = projected.reshape(3, shard_total, PACK_DEV, HEADS, HEAD)
        attended = lax.map(shard_attention, (shaped[0], shaped[1], shaped[2], labels.reshape(shard_total, PACK_DEV)))
        attended = attended.reshape(PACKED, D)
        residual = stream.astype(jnp.float32) + split_sum(attended, w_o[layer_index], N_MP) + b_o[layer_index]
        normed_mlp = layer_norm(residual, ln_gain[layer_index, 1], ln_bias[layer_index, 1])
        up_proj = jnp.dot(normed_mlp, w_up[layer_index], preferred_element_type=jnp.float32) + b_up[layer_index]
        hidden = jax.nn.gelu(up_proj, approximate=False).astype(jnp.bfloat16)
        stream = (residual + split_sum(hidden, w_down[layer_index], N_MP) + b_down[layer_index]).astype(jnp.bfloat16)
    return jnp.where(labels[:, None] >= 0, stream, jnp.zeros_like(stream))
```

```python
import functools
import math

import jax
import jax.numpy as jnp
from jax import lax
from jax.experimental import pallas as pl
from jax.experimental.pallas import tpu as pltpu
from jax.sharding import PartitionSpec as P

HEAD = 80
MESH = pl.DeviceIdType.MESH


def norm_rows(values, gain_row, shift_row):
    row_mean = jnp.mean(values, axis=-1, keepdims=True)
    centred = values - row_mean
    spread = jnp.mean(centred * centred, axis=-1, keepdims=True)
    return (centred * lax.rsqrt(spread + 1e-06) * gain_row + shift_row).astype(jnp.bfloat16)


def flip(index, mask, count):
    result = index
    bit = 1
    while bit < count:
        wanted = (mask // bit) % 2
        own = (index // bit) % 2
        result = result + bit * wanted * (1 - 2 * own)
        bit = bit * 2
    return result


def tile_of(extent, most):
    tile = most
    while extent % tile != 0:
        tile = tile // 2
    return tile


def route_kernel(shards, groups, packed_ref, out_ref, send_sem, recv_sem, own_sem):
    per = shards // groups
    dp = lax.axis_index("dp")
    mp = lax.axis_index("mp")
    home = dp // per
    slot = lax.rem(dp, per) * groups + mp

    barrier = pltpu.get_barrier_semaphore()
    for j in range(per):
        for g in range(groups):
            source = mp * per + j

            @pl.when(jnp.logical_or(source != dp, mp != g))
            def _():
                pl.semaphore_signal(barrier, inc=1, device_id=(source, g), device_id_type=MESH)

    is_home = home == mp

    @pl.when(is_home)
    def _():
        pl.semaphore_wait(barrier, shards - 1)

    @pl.when(jnp.logical_not(is_home))
    def _():
        pl.semaphore_wait(barrier, shards)

    def remote(step):
        dest = lax.rem(dp + step, shards)
        return pltpu.make_async_remote_copy(
            src_ref=packed_ref.at[dest],
            dst_ref=out_ref.at[slot],
            send_sem=send_sem.at[step],
            recv_sem=recv_sem.at[slot],
            device_id=(dest, home),
            device_id_type=MESH,
        )

    own = pltpu.make_async_copy(packed_ref.at[dp], out_ref.at[slot], own_sem)
    for step in range(1, shards):
        remote(step).start()

    @pl.when(is_home)
    def _():
        own.start()
        own.wait()

    @pl.when(jnp.logical_not(is_home))
    def _():
        remote(0).start()
        remote(0).wait_send()

    for step in range(1, shards):
        remote(step).wait_send()
    for j in range(per):
        for g in range(groups):
            source = mp * per + j

            @pl.when(jnp.logical_or(source != dp, mp != g))
            def _():
                pltpu.make_async_remote_copy(
                    src_ref=packed_ref.at[0],
                    dst_ref=out_ref.at[j * groups + g],
                    send_sem=send_sem.at[0],
                    recv_sem=recv_sem.at[j * groups + g],
                    device_id=(dp, mp),
                    device_id_type=MESH,
                ).wait_recv()


def route(packed, shards, groups):
    vmem = pl.BlockSpec(memory_space=pltpu.VMEM)
    return pl.pallas_call(
        functools.partial(route_kernel, shards, groups),
        out_shape=jax.ShapeDtypeStruct(packed.shape, packed.dtype),
        in_specs=[vmem],
        out_specs=vmem,
        scratch_shapes=[
            pltpu.SemaphoreType.DMA((shards,)),
            pltpu.SemaphoreType.DMA((shards,)),
            pltpu.SemaphoreType.DMA,
        ],
        compiler_params=pltpu.CompilerParams(collective_id=0, has_side_effects=True),
        cost_estimate=pl.CostEstimate(flops=15_000_000_000, bytes_accessed=0, transcendentals=0),
        name="route",
    )(packed)


def exchange(groups, x_ref, blocks, parts, backs, sems, block_step, finish):
    own_sem, send_a, recv_a, send_b, recv_b = sems
    dp = lax.axis_index("dp")
    mp = lax.axis_index("mp")

    barrier = pltpu.get_barrier_semaphore()
    for k in range(1, groups):
        pl.semaphore_signal(
            barrier, inc=1, device_id=(dp, flip(mp, k, groups)), device_id_type=MESH
        )
    own = pltpu.make_async_copy(x_ref, blocks.at[0], own_sem)
    own.start()
    pl.semaphore_wait(barrier, groups - 1)

    def out_copy(k):
        return pltpu.make_async_remote_copy(
            src_ref=x_ref,
            dst_ref=blocks.at[k],
            send_sem=send_a.at[k],
            recv_sem=recv_a.at[k],
            device_id=(dp, flip(mp, k, groups)),
            device_id_type=MESH,
        )

    def back_copy(k):
        return pltpu.make_async_remote_copy(
            src_ref=parts.at[k],
            dst_ref=backs.at[k],
            send_sem=send_b.at[k],
            recv_sem=recv_b.at[k],
            device_id=(dp, flip(mp, k, groups)),
            device_id_type=MESH,
        )

    for k in range(1, groups):
        out_copy(k).start()
    own.wait()

    def step(k, carry):
        @pl.when(k > 0)
        def _():
            out_copy(k).wait_recv()

        block_step(k, flip(mp, k, groups))

        @pl.when(k > 0)
        def _():
            back_copy(k).start()

        return carry

    lax.fori_loop(0, groups, step, 0)
    for k in range(1, groups):
        back_copy(k).wait_recv()
    finish()
    for k in range(1, groups):
        out_copy(k).wait_send()
        back_copy(k).wait_send()


def sum_parts(groups, parts, backs, rows):
    total = parts[0, rows, :].astype(jnp.float32)
    for k in range(1, groups):
        total = total + backs[k, rows, :].astype(jnp.float32)
    return total


def attention_kernel(
    groups,
    x_ref,
    stream_ref,
    w_ref,
    b_ref,
    label_col_ref,
    label_row_ref,
    bias_ref,
    gain_ref,
    shift_ref,
    residual_ref,
    normed_ref,
    blocks,
    parts,
    backs,
    attended_ref,
    *sems,
):
    row_count, depth = x_ref.shape
    width = w_ref.shape[2]
    heads = width // HEAD
    scale = 1.0 / math.sqrt(HEAD)
    tile = tile_of(depth, 256)

    def block_step(k, source):
        x = blocks[k]

        def project(t):
            y = jnp.dot(x, w_ref[t], preferred_element_type=jnp.float32)
            return (y + b_ref[t]).astype(jnp.bfloat16)

        query, key, value = project(0), project(1), project(2)
        matches = label_col_ref[source] == label_row_ref[source]
        lane_head = lax.broadcasted_iota(jnp.int32, (row_count, width), 1)
        total = jnp.zeros((row_count, width), jnp.float32)
        zero = jnp.zeros((row_count, width), jnp.bfloat16)
        for h in range(heads):
            inside = (lane_head >= h * HEAD) & (lane_head < (h + 1) * HEAD)
            scores = lax.dot_general(
                jnp.where(inside, query, zero),
                key,
                (((1,), (1,)), ((), ())),
                preferred_element_type=jnp.float32,
            )
            scores = jnp.where(matches, scores * scale, -jnp.inf)
            weights = jnp.exp(scores - jnp.max(scores, axis=-1, keepdims=True))
            inverse = 1.0 / jnp.sum(weights, axis=-1, keepdims=True)
            probabilities = (weights * inverse).astype(jnp.bfloat16)
            total = total + jnp.dot(
                probabilities, jnp.where(inside, value, zero), preferred_element_type=jnp.float32
            )
        attended_ref[...] = total.astype(jnp.bfloat16)

        def column(t, carry):
            at = pl.ds(pl.multiple_of(t * tile, tile), tile)
            parts[k, :, at] = lax.dot_general(
                attended_ref[...],
                w_ref[3, at, :],
                (((1,), (1,)), ((), ())),
                preferred_element_type=jnp.float32,
            ).astype(jnp.bfloat16)
            return carry

        lax.fori_loop(0, depth // tile, column, 0)

    def finish():
        rows_tile = tile_of(row_count, 32)

        def some(i, carry):
            rows = pl.ds(pl.multiple_of(i * rows_tile, rows_tile), rows_tile)
            residual = (
                stream_ref[rows, :].astype(jnp.float32)
                + sum_parts(groups, parts, backs, rows)
                + bias_ref[...]
            )
            residual_ref[rows, :] = residual
            normed_ref[rows, :] = norm_rows(residual, gain_ref[...], shift_ref[...])
            return carry

        lax.fori_loop(0, row_count // rows_tile, some, 0)

    exchange(groups, x_ref, blocks, parts, backs, sems, block_step, finish)


def mlp_kernel(
    groups,
    x_ref,
    residual_ref,
    up_ref,
    b_ref,
    down_ref,
    bias_ref,
    out_ref,
    blocks,
    parts,
    backs,
    hidden_ref,
    *sems,
):
    row_count, depth = x_ref.shape
    width = up_ref.shape[1]
    tile = tile_of(depth, 256)
    up_tile = tile_of(width, 256)

    def block_step(k, source):
        def up(t, carry):
            at = pl.ds(pl.multiple_of(t * up_tile, up_tile), up_tile)
            y = jnp.dot(blocks[k], up_ref[:, at], preferred_element_type=jnp.float32) + b_ref[:, at]
            y = 0.5 * y * (1.0 + lax.erf(y * math.sqrt(0.5)))
            hidden_ref[:, at] = y.astype(jnp.bfloat16)
            return carry

        lax.fori_loop(0, width // up_tile, up, 0)

        def column(t, carry):
            at = pl.ds(pl.multiple_of(t * tile, tile), tile)
            parts[k, :, at] = jnp.dot(
                hidden_ref[...], down_ref[:, at], preferred_element_type=jnp.float32
            ).astype(jnp.bfloat16)
            return carry

        lax.fori_loop(0, depth // tile, column, 0)

    def finish():
        rows_tile = tile_of(row_count, 32)

        def some(i, carry):
            rows = pl.ds(pl.multiple_of(i * rows_tile, rows_tile), rows_tile)
            out_ref[rows, :] = (
                residual_ref[rows, :] + sum_parts(groups, parts, backs, rows) + bias_ref[...]
            ).astype(jnp.bfloat16)
            return carry

        lax.fori_loop(0, row_count // rows_tile, some, 0)

    exchange(groups, x_ref, blocks, parts, backs, sems, block_step, finish)


def exchange_call(kernel, groups, args, outs, width, collective_id, name):
    row_count, depth = args[0].shape
    vmem = pl.BlockSpec(memory_space=pltpu.VMEM)
    many = pltpu.SemaphoreType.DMA((groups,))
    return pl.pallas_call(
        functools.partial(kernel, groups),
        out_shape=outs,
        in_specs=[vmem] * len(args),
        out_specs=jax.tree.map(lambda _: vmem, outs),
        scratch_shapes=[
            pltpu.VMEM((groups, row_count, depth), jnp.bfloat16),
            pltpu.VMEM((groups, row_count, depth), jnp.bfloat16),
            pltpu.VMEM((groups, row_count, depth), jnp.bfloat16),
            pltpu.VMEM((row_count, width), jnp.bfloat16),
            pltpu.SemaphoreType.DMA,
            many,
            many,
            many,
            many,
        ],
        compiler_params=pltpu.CompilerParams(
            collective_id=collective_id, has_side_effects=True, vmem_limit_bytes=48 * 1024 * 1024
        ),
        cost_estimate=pl.CostEstimate(flops=50_000_000_000, bytes_accessed=0, transcendentals=0),
        name=name,
    )(*args)


def per_device(
    patches,
    position,
    keep,
    counts,
    offsets,
    ln_gain,
    ln_bias,
    w_qkv,
    b_qkv,
    w_o,
    b_o,
    w_up,
    b_up,
    w_down,
    b_down,
):
    local_images, patch_count, column_count = patches.shape
    keep_most = keep.shape[1]
    shard_count = lax.axis_size("dp")
    group_size = lax.axis_size("mp")
    images_here = local_images * group_size
    per_slot = (images_here + shard_count - 1) // shard_count
    slot_rows = max(keep_most + 16, per_slot * keep_most * 5 // 8)
    pack_rows = slot_rows * shard_count
    local_rows = pack_rows // group_size
    dp_index = lax.axis_index("dp")
    mp_index = lax.axis_index("mp")
    f32 = jnp.float32

    attention_shard = jnp.concatenate([w_qkv[0], w_o[0].T[None]], axis=0)
    w_attention = lax.all_gather(attention_shard, "dp", axis=1, tiled=True)
    w_up_full = lax.all_gather(w_up[0], "dp", axis=0, tiled=True)
    w_down_full = lax.all_gather(w_down[0], "dp", axis=1, tiled=True)

    chosen = (keep[:, :, None] == jnp.arange(patch_count, dtype=jnp.int32)).astype(jnp.bfloat16)
    tokens = (
        jnp.einsum("ijp,ipd->ijd", chosen, patches, preferred_element_type=f32)
        + jnp.einsum("ijp,pd->ijd", chosen, position, preferred_element_type=f32)
    ).astype(jnp.bfloat16)

    first_image = dp_index * images_here
    group_counts = lax.dynamic_slice_in_dim(counts, first_image, images_here)
    group_offsets = lax.dynamic_slice_in_dim(offsets, first_image, images_here)
    positions_in = jnp.arange(keep_most, dtype=jnp.int32)
    group_live = positions_in[None, :] < group_counts[:, None]
    shard_index = group_offsets // pack_rows
    base_row = (
        shard_index * slot_rows + group_offsets - shard_index * pack_rows - dp_index * slot_rows
    )
    target = jnp.where(group_live, base_row[:, None] + positions_in[None, :], pack_rows).reshape(-1)
    image_ids = jnp.arange(counts.shape[0], dtype=jnp.int32)
    packed_rows = dp_index * pack_rows + jnp.arange(pack_rows, dtype=jnp.int32)
    inside = (packed_rows[:, None] >= offsets[None, :]) & (
        packed_rows[:, None] < (offsets + counts)[None, :]
    )
    labels = jnp.max(jnp.where(inside, image_ids[None, :] + 1, 0), axis=1) - 1

    featured = lax.all_to_all(
        tokens.reshape(-1, column_count), "mp", split_axis=1, concat_axis=0, tiled=True
    )
    feature_count = featured.shape[1]
    placing = (jnp.arange(pack_rows, dtype=jnp.int32)[:, None] == target[None, :]).astype(
        jnp.bfloat16
    )
    packed = jnp.dot(placing, featured, preferred_element_type=f32).astype(jnp.bfloat16)
    arrived = route(
        packed.reshape(shard_count, slot_rows, feature_count), shard_count, group_size
    )
    per = shard_count // group_size
    stream = (
        arrived.reshape(per, group_size, slot_rows, feature_count)
        .transpose(0, 2, 1, 3)
        .reshape(local_rows, column_count)
    )
    normed = norm_rows(stream.astype(f32), ln_gain[0, 0], ln_bias[0, 0])
    by_group = labels.reshape(group_size, local_rows)
    residual, normed_mlp = exchange_call(
        attention_kernel,
        group_size,
        (
            normed,
            stream,
            w_attention,
            b_qkv[0][:, None, :],
            by_group[:, :, None],
            by_group[:, None, :],
            b_o,
            ln_gain[:, 1],
            ln_bias[:, 1],
        ),
        (
            jax.ShapeDtypeStruct((local_rows, column_count), f32),
            jax.ShapeDtypeStruct((local_rows, column_count), jnp.bfloat16),
        ),
        w_attention.shape[2],
        1,
        "attention",
    )
    stream = exchange_call(
        mlp_kernel,
        group_size,
        (normed_mlp, residual, w_up_full, b_up, w_down_full, b_down),
        jax.ShapeDtypeStruct((local_rows, column_count), jnp.bfloat16),
        w_up_full.shape[1],
        2,
        "mlp",
    )
    own_labels = lax.dynamic_slice_in_dim(labels, mp_index * local_rows, local_rows)
    return jnp.where(own_labels[:, None] >= 0, stream, jnp.zeros_like(stream))


def solution(mesh):
    in_specs = (
        P(("dp", "mp"), None, None),
        P(),
        P(("dp", "mp"), None),
        P(),
        P(),
        P(),
        P(),
        P(None, None, "dp", "mp"),
        P(None, None, "mp"),
        P(None, "mp", "dp"),
        P(),
        P(None, "dp", "mp"),
        P(None, "mp"),
        P(None, "mp", "dp"),
        P(),
    )
    out_specs = P(("dp", "mp"), None)
    return jax.shard_map(
        per_device, mesh=mesh, in_specs=in_specs, out_specs=out_specs, check_vma=False
    )
```

```python
import functools
import math

import jax
import jax.numpy as jnp
from jax import lax
from jax.experimental import pallas as pl
from jax.experimental.pallas import tpu as pltpu
from jax.sharding import PartitionSpec as P

HEAD = 80
MESH = pl.DeviceIdType.MESH


def norm_rows(values, gain_row, shift_row):
    row_mean = jnp.mean(values, axis=-1, keepdims=True)
    centred = values - row_mean
    spread = jnp.mean(centred * centred, axis=-1, keepdims=True)
    return (centred * lax.rsqrt(spread + 1e-06) * gain_row + shift_row).astype(jnp.bfloat16)


def flip(index, mask, count):
    result = index
    bit = 1
    while bit < count:
        wanted = (mask // bit) % 2
        own = (index // bit) % 2
        result = result + bit * wanted * (1 - 2 * own)
        bit = bit * 2
    return result


def tile_of(extent, most):
    tile = most
    while extent % tile != 0:
        tile = tile // 2
    return tile


def route_kernel(
    shards,
    groups,
    packed_ref,
    gain_ref,
    shift_ref,
    stream_ref,
    normed_ref,
    out_ref,
    send_sem,
    recv_sem,
    own_sem,
):
    per = shards // groups
    dp = lax.axis_index("dp")
    mp = lax.axis_index("mp")
    home = dp // per
    slot = lax.rem(dp, per) * groups + mp

    barrier = pltpu.get_barrier_semaphore()
    for j in range(per):
        for g in range(groups):
            source = mp * per + j

            @pl.when(jnp.logical_or(source != dp, mp != g))
            def _():
                pl.semaphore_signal(barrier, inc=1, device_id=(source, g), device_id_type=MESH)

    is_home = home == mp

    @pl.when(is_home)
    def _():
        pl.semaphore_wait(barrier, shards - 1)

    @pl.when(jnp.logical_not(is_home))
    def _():
        pl.semaphore_wait(barrier, shards)

    def remote(step):
        dest = lax.rem(dp + step, shards)
        return pltpu.make_async_remote_copy(
            src_ref=packed_ref.at[dest],
            dst_ref=out_ref.at[slot],
            send_sem=send_sem.at[step],
            recv_sem=recv_sem.at[slot],
            device_id=(dest, home),
            device_id_type=MESH,
        )

    own = pltpu.make_async_copy(packed_ref.at[dp], out_ref.at[slot], own_sem)
    for step in range(1, shards):
        remote(step).start()

    @pl.when(is_home)
    def _():
        own.start()
        own.wait()

    @pl.when(jnp.logical_not(is_home))
    def _():
        remote(0).start()
        remote(0).wait_send()

    for step in range(1, shards):
        remote(step).wait_send()
    for j in range(per):
        for g in range(groups):
            source = mp * per + j

            @pl.when(jnp.logical_or(source != dp, mp != g))
            def _():
                pltpu.make_async_remote_copy(
                    src_ref=packed_ref.at[0],
                    dst_ref=out_ref.at[j * groups + g],
                    send_sem=send_sem.at[0],
                    recv_sem=recv_sem.at[j * groups + g],
                    device_id=(dp, mp),
                    device_id_type=MESH,
                ).wait_recv()

    rows_tile = tile_of(packed_ref.shape[1], 32)
    for j in range(per):

        def some(i, carry):
            rows = pl.ds(pl.multiple_of(i * rows_tile, rows_tile), rows_tile)
            whole = jnp.concatenate(
                [out_ref[j * groups + g, rows, :] for g in range(groups)], axis=-1
            )
            stream_ref[j, rows, :] = whole
            normed_ref[j, rows, :] = norm_rows(
                whole.astype(jnp.float32), gain_ref[...], shift_ref[...]
            )
            return carry

        lax.fori_loop(0, packed_ref.shape[1] // rows_tile, some, 0)


def route(packed, gain_row, shift_row, shards, groups):
    slot_rows, width = packed.shape[1:]
    result = jax.ShapeDtypeStruct((shards // groups, slot_rows, width * groups), packed.dtype)
    vmem = pl.BlockSpec(memory_space=pltpu.VMEM)
    return pl.pallas_call(
        functools.partial(route_kernel, shards, groups),
        out_shape=(result, result),
        in_specs=[vmem] * 3,
        out_specs=(vmem, vmem),
        scratch_shapes=[
            pltpu.VMEM(packed.shape, packed.dtype),
            pltpu.SemaphoreType.DMA((shards,)),
            pltpu.SemaphoreType.DMA((shards,)),
            pltpu.SemaphoreType.DMA,
        ],
        compiler_params=pltpu.CompilerParams(collective_id=0, has_side_effects=True),
        cost_estimate=pl.CostEstimate(flops=15_000_000_000, bytes_accessed=0, transcendentals=0),
        name="route",
    )(packed, gain_row, shift_row)


def exchange(groups, x_ref, blocks, parts, backs, relay, sems, block_step, finish):
    own_sem, send_a, recv_a, send_b, recv_b = sems
    dp = lax.axis_index("dp")
    mp = lax.axis_index("mp")
    pieces = x_ref.shape[0]
    square = groups == 4 and pieces == 2
    partners = range(1, 3) if square else range(1, groups)

    barrier = pltpu.get_barrier_semaphore()
    for k in partners:
        pl.semaphore_signal(
            barrier, inc=1, device_id=(dp, flip(mp, k, groups)), device_id_type=MESH
        )
    own = pltpu.make_async_copy(x_ref, blocks.at[pl.ds(0, pieces)], own_sem)
    own.start()
    pl.semaphore_wait(barrier, len(partners))

    def send(source, target, out_sem, in_sem, k):
        return pltpu.make_async_remote_copy(
            src_ref=source,
            dst_ref=target,
            send_sem=out_sem,
            recv_sem=in_sem,
            device_id=(dp, flip(mp, k, groups)),
            device_id_type=MESH,
        )

    def out_copy(k, h):
        at = k * pieces + h
        return send(x_ref.at[h], blocks.at[at], send_a.at[at], recv_a.at[at], k)

    def back_copy(k, h):
        at = k * pieces + h
        return send(parts.at[at], backs.at[at], send_b.at[at], recv_b.at[at], k)

    if square:
        def forward(h):
            held, k = (2, 2) if h == 0 else (5, 1)
            at = 6 + h
            return send(blocks.at[held], blocks.at[at], send_a.at[at], recv_a.at[at], k)

        def across(h):
            at = 6 + h
            return send(parts.at[at], relay.at[h], send_b.at[at], recv_b.at[at], 1 + h)

        for k, h in ((1, 0), (2, 1), (1, 1), (2, 0)):
            out_copy(k, h).start()
        own.wait()

        def step(i, carry):
            late = (i + 2) // 8
            middle = ((i + 2) // 4) % 2
            k = middle * (1 + i % 2) + 3 * late
            h = (i // 4 + i % 2) % 2

            @pl.when(i == 2)
            def _():
                out_copy(1, 0).wait_recv()
                forward(0).start()
                out_copy(2, 1).wait_recv()
                forward(1).start()

            @pl.when(i >= 4)
            def _():
                out_copy(k, h).wait_recv()

            block_step(k * 2 + h, flip(mp, k, groups) * 2 + h)

            @pl.when(i == 2)
            def _():
                back_copy(1, 0).start()

            @pl.when(i == 3)
            def _():
                back_copy(2, 1).start()

            @pl.when(i == 6)
            def _():
                across(1).start()

            @pl.when(i == 7)
            def _():
                across(0).start()

            return carry

        lax.fori_loop(0, 8, step, 0)
        rows_tile = tile_of(x_ref.shape[1], 32)
        for h, k in ((1, 1), (0, 2)):
            across(h).wait_recv()

            def add(i, carry, h=h, k=k):
                rows = pl.ds(pl.multiple_of(i * rows_tile, rows_tile), rows_tile)
                parts[k * 2 + h, rows, :] = (
                    parts[k * 2 + h, rows, :].astype(jnp.float32)
                    + relay[h, rows, :].astype(jnp.float32)
                ).astype(jnp.bfloat16)
                return carry

            lax.fori_loop(0, x_ref.shape[1] // rows_tile, add, 0)
            back_copy(k, h).start()
        for k, h in ((1, 0), (2, 1), (1, 1), (2, 0)):
            back_copy(k, h).wait_recv()
        finish(partners)
        for h in range(2):
            forward(h).wait_send()
            across(h).wait_send()
            for k in partners:
                out_copy(k, h).wait_send()
                back_copy(k, h).wait_send()
        return

    for k in partners:
        for h in range(pieces):
            out_copy(k, h).start()
    own.wait()

    def step(i, carry):
        k = i // pieces
        h = i % pieces

        @pl.when(k > 0)
        def _():
            out_copy(k, h).wait_recv()

        block_step(i, flip(mp, k, groups) * pieces + h)

        @pl.when(k > 0)
        def _():
            back_copy(k, h).start()

        return carry

    lax.fori_loop(0, groups * pieces, step, 0)
    for k in partners:
        for h in range(pieces):
            back_copy(k, h).wait_recv()
    finish(partners)
    for k in partners:
        for h in range(pieces):
            out_copy(k, h).wait_send()
            back_copy(k, h).wait_send()


def finish_rows(x_ref, parts, backs, partners, write):
    pieces, row_count = x_ref.shape[:2]
    rows_tile = tile_of(row_count, 32)
    for h in range(pieces):

        def some(i, carry, h=h):
            rows = pl.ds(pl.multiple_of(i * rows_tile, rows_tile), rows_tile)
            total = parts[h, rows, :].astype(jnp.float32)
            for k in partners:
                total = total + backs[k * pieces + h, rows, :].astype(jnp.float32)
            write(h, rows, total)
            return carry

        lax.fori_loop(0, row_count // rows_tile, some, 0)


def attention_kernel(
    groups,
    x_ref,
    stream_ref,
    w_ref,
    b_ref,
    label_col_ref,
    label_row_ref,
    bias_ref,
    gain_ref,
    shift_ref,
    residual_ref,
    normed_ref,
    blocks,
    parts,
    backs,
    relay,
    attended_ref,
    *sems,
):
    row_count, depth = x_ref.shape[1:]
    width = w_ref.shape[2]
    heads = width // HEAD
    scale = 1.0 / math.sqrt(HEAD)
    tile = tile_of(depth, 256)

    def block_step(at_block, source):
        x = blocks[at_block]

        def project(t):
            y = jnp.dot(x, w_ref[t], preferred_element_type=jnp.float32)
            return (y + b_ref[t]).astype(jnp.bfloat16)

        query, key, value = project(0), project(1), project(2)
        matches = label_col_ref[source] == label_row_ref[source]
        lane_head = lax.broadcasted_iota(jnp.int32, (row_count, width), 1)
        total = jnp.zeros((row_count, width), jnp.float32)
        zero = jnp.zeros((row_count, width), jnp.bfloat16)
        for h in range(heads):
            inside = (lane_head >= h * HEAD) & (lane_head < (h + 1) * HEAD)
            scores = lax.dot_general(
                jnp.where(inside, query, zero),
                key,
                (((1,), (1,)), ((), ())),
                preferred_element_type=jnp.float32,
            )
            scores = jnp.where(matches, scores * scale, -jnp.inf)
            weights = jnp.exp(scores - jnp.max(scores, axis=-1, keepdims=True))
            inverse = 1.0 / jnp.sum(weights, axis=-1, keepdims=True)
            probabilities = (weights * inverse).astype(jnp.bfloat16)
            total = total + jnp.dot(
                probabilities, jnp.where(inside, value, zero), preferred_element_type=jnp.float32
            )
        attended_ref[...] = total.astype(jnp.bfloat16)

        def column(t, carry):
            at = pl.ds(pl.multiple_of(t * tile, tile), tile)
            parts[at_block, :, at] = lax.dot_general(
                attended_ref[...],
                w_ref[3, at, :],
                (((1,), (1,)), ((), ())),
                preferred_element_type=jnp.float32,
            ).astype(jnp.bfloat16)
            return carry

        lax.fori_loop(0, depth // tile, column, 0)

    def finish(partners):
        def write(h, rows, total):
            residual = stream_ref[h, rows, :].astype(jnp.float32) + total + bias_ref[...]
            residual_ref[h, rows, :] = residual
            normed_ref[h, rows, :] = norm_rows(residual, gain_ref[...], shift_ref[...])

        finish_rows(x_ref, parts, backs, partners, write)

    exchange(groups, x_ref, blocks, parts, backs, relay, sems, block_step, finish)


def mlp_kernel(
    groups,
    x_ref,
    residual_ref,
    up_ref,
    b_ref,
    down_ref,
    bias_ref,
    out_ref,
    blocks,
    parts,
    backs,
    relay,
    hidden_ref,
    *sems,
):
    row_count, depth = x_ref.shape[1:]
    width = up_ref.shape[1]
    tile = tile_of(depth, 256)
    up_tile = tile_of(width, 256)

    def block_step(at_block, source):
        def up(t, carry):
            at = pl.ds(pl.multiple_of(t * up_tile, up_tile), up_tile)
            y = jnp.dot(blocks[at_block], up_ref[:, at], preferred_element_type=jnp.float32) + b_ref[:, at]
            y = 0.5 * y * (1.0 + lax.erf(y * math.sqrt(0.5)))
            hidden_ref[:, at] = y.astype(jnp.bfloat16)
            return carry

        lax.fori_loop(0, width // up_tile, up, 0)

        def column(t, carry):
            at = pl.ds(pl.multiple_of(t * tile, tile), tile)
            parts[at_block, :, at] = lax.dot_general(
                hidden_ref[...],
                down_ref[at, :],
                (((1,), (1,)), ((), ())),
                preferred_element_type=jnp.float32,
            ).astype(jnp.bfloat16)
            return carry

        lax.fori_loop(0, depth // tile, column, 0)

    def finish(partners):
        def write(h, rows, total):
            out_ref[h, rows, :] = (residual_ref[h, rows, :] + total + bias_ref[...]).astype(
                jnp.bfloat16
            )

        finish_rows(x_ref, parts, backs, partners, write)

    exchange(groups, x_ref, blocks, parts, backs, relay, sems, block_step, finish)


def exchange_call(kernel, groups, args, outs, width, collective_id, name):
    pieces, row_count, depth = args[0].shape
    vmem = pl.BlockSpec(memory_space=pltpu.VMEM)
    many = pltpu.SemaphoreType.DMA((groups * pieces,))
    buffer = pltpu.VMEM((groups * pieces, row_count, depth), jnp.bfloat16)
    return pl.pallas_call(
        functools.partial(kernel, groups),
        out_shape=outs,
        in_specs=[vmem] * len(args),
        out_specs=jax.tree.map(lambda _: vmem, outs),
        scratch_shapes=[
            buffer,
            buffer,
            buffer,
            pltpu.VMEM((pieces, row_count, depth), jnp.bfloat16),
            pltpu.VMEM((row_count, width), jnp.bfloat16),
            pltpu.SemaphoreType.DMA,
            many,
            many,
            many,
            many,
        ],
        compiler_params=pltpu.CompilerParams(
            collective_id=collective_id, has_side_effects=True, vmem_limit_bytes=48 * 1024 * 1024
        ),
        cost_estimate=pl.CostEstimate(flops=50_000_000_000, bytes_accessed=0, transcendentals=0),
        name=name,
    )(*args)


def per_device(
    patches,
    position,
    keep,
    counts,
    offsets,
    ln_gain,
    ln_bias,
    w_qkv,
    b_qkv,
    w_o,
    b_o,
    w_up,
    b_up,
    w_down,
    b_down,
):
    local_images, patch_count, column_count = patches.shape
    keep_most = keep.shape[1]
    shard_count = lax.axis_size("dp")
    group_size = lax.axis_size("mp")
    images_here = local_images * group_size
    per_slot = (images_here + shard_count - 1) // shard_count
    slot_rows = max(keep_most + 16, per_slot * keep_most * 5 // 8)
    pack_rows = slot_rows * shard_count
    local_rows = pack_rows // group_size
    dp_index = lax.axis_index("dp")
    mp_index = lax.axis_index("mp")
    f32 = jnp.float32

    attention_shard = jnp.concatenate([w_qkv[0], w_o[0].T[None]], axis=0)
    w_attention = lax.all_gather(attention_shard, "dp", axis=1, tiled=True)

    chosen = (keep[:, :, None] == jnp.arange(patch_count, dtype=jnp.int32)).astype(jnp.bfloat16)
    tokens = (
        jnp.einsum("ijp,ipd->ijd", chosen, patches, preferred_element_type=f32)
        + jnp.einsum("ijp,pd->ijd", chosen, position, preferred_element_type=f32)
    ).astype(jnp.bfloat16)
    tokens, w_up_shard = lax.optimization_barrier((tokens, w_up[0]))
    w_up_full = lax.all_gather(w_up_shard, "dp", axis=0, tiled=True)

    first_image = dp_index * images_here
    group_counts = lax.dynamic_slice_in_dim(counts, first_image, images_here)
    group_offsets = lax.dynamic_slice_in_dim(offsets, first_image, images_here)
    positions_in = jnp.arange(keep_most, dtype=jnp.int32)
    group_live = positions_in[None, :] < group_counts[:, None]
    shard_index = group_offsets // pack_rows
    base_row = (
        shard_index * slot_rows + group_offsets - shard_index * pack_rows - dp_index * slot_rows
    )
    target = jnp.where(group_live, base_row[:, None] + positions_in[None, :], pack_rows).reshape(-1)
    image_ids = jnp.arange(counts.shape[0], dtype=jnp.int32)
    packed_rows = dp_index * pack_rows + jnp.arange(pack_rows, dtype=jnp.int32)
    inside = (packed_rows[:, None] >= offsets[None, :]) & (
        packed_rows[:, None] < (offsets + counts)[None, :]
    )
    labels = jnp.max(jnp.where(inside, image_ids[None, :] + 1, 0), axis=1) - 1

    featured = lax.all_to_all(
        tokens.reshape(-1, column_count), "mp", split_axis=1, concat_axis=0, tiled=True
    )
    featured, w_down_shard = lax.optimization_barrier((featured, w_down[0]))
    w_down_rows = lax.all_gather(w_down_shard, "dp", axis=1, tiled=True).T
    feature_count = featured.shape[1]
    placing = (jnp.arange(pack_rows, dtype=jnp.int32)[:, None] == target[None, :]).astype(
        jnp.bfloat16
    )
    packed = jnp.dot(placing, featured, preferred_element_type=f32).astype(jnp.bfloat16)
    stream, normed = route(
        packed.reshape(shard_count, slot_rows, feature_count),
        ln_gain[:, 0],
        ln_bias[:, 0],
        shard_count,
        group_size,
    )
    pieces = stream.shape[0]
    by_piece = labels.reshape(group_size * pieces, local_rows // pieces)
    residual, normed_mlp = exchange_call(
        attention_kernel,
        group_size,
        (
            normed,
            stream,
            w_attention,
            b_qkv[0][:, None, :],
            by_piece[:, :, None],
            by_piece[:, None, :],
            b_o,
            ln_gain[:, 1],
            ln_bias[:, 1],
        ),
        (
            jax.ShapeDtypeStruct(stream.shape, f32),
            jax.ShapeDtypeStruct(stream.shape, jnp.bfloat16),
        ),
        w_attention.shape[2],
        1,
        "attention",
    )
    stream = exchange_call(
        mlp_kernel,
        group_size,
        (normed_mlp, residual, w_up_full, b_up, w_down_rows, b_down),
        jax.ShapeDtypeStruct(stream.shape, jnp.bfloat16),
        w_up_full.shape[1],
        2,
        "mlp",
    ).reshape(local_rows, column_count)
    own_labels = lax.dynamic_slice_in_dim(labels, mp_index * local_rows, local_rows)
    return jnp.where(own_labels[:, None] >= 0, stream, jnp.zeros_like(stream))


def solution(mesh):
    in_specs = (
        P(("dp", "mp"), None, None),
        P(),
        P(("dp", "mp"), None),
        P(),
        P(),
        P(),
        P(),
        P(None, None, "dp", "mp"),
        P(None, None, "mp"),
        P(None, "mp", "dp"),
        P(),
        P(None, "dp", "mp"),
        P(None, "mp"),
        P(None, "mp", "dp"),
        P(),
    )
    out_specs = P(("dp", "mp"), None)
    return jax.shard_map(
        per_device, mesh=mesh, in_specs=in_specs, out_specs=out_specs, check_vma=False
    )
```
